512 devices in a mesh: row: 16 (over z), col: 32 (over x, y, core).
Axes of the slice: x: 4, y: 4, z: 16, core: 2. Of those that a mesh axis runs over, the one named last changes fastest.
Arguments:
- rhs_panels: float32 [3, 16, 32, 64, 256], P(None, 'row', 'col'), may hold values from -6 to 6
- inverse_diag: bfloat16 [3, 16, 32, 256, 256], P(None, 'row', 'col'), may hold values from -0.375 to 0.375
- factor_blocks: bfloat16 [3, 16, 320, 256, 256], P(None, 'row', 'col'), may hold values from -0.078125 to 0.078125
- block_target: int32 [3, 16, 320], P(None, 'row', 'col'), may hold values from 0 to 15, as said below
- block_source: int32 [3, 16, 320], P(None, 'row', 'col'), may hold values from 0 to 31, as said below
Outputs:
- solution: float32 [3, 16, 32, 64, 256], P(None, 'row', 'col')
The draws below stay inside these ranges and needn't reach their ends.
Inputs may be any that keep to these rules, and one draw needn't show every extreme that they name: (block_target[p, r, q] - r) modulo 16 is below 2, or equals 8, or equals 15; each of 1, 8 and 15 occurs. (block_source[p, r, q] - q // 10) modulo 32 is below 2, or equals 16, or equals 31; each of 1, 16 and 31 occurs.
All inputs are finite; a program needn't handle non-finite values.
Results may differ from the reference program's by a relative error of at most 0.014.
Values may be sent and summed in bfloat16 or wider, within the bound.
No kernel may reach another device: no remote copies, remote signals or barrier semaphores. Data moves between devices by JAX's collectives and lax.ppermute only.
A program may use at most 64 MiB of HBM per device.

```python
import jax
import jax.numpy as jnp
from jax import lax

BS = 256
NRHS = 64
LEVELS = 3
WINDOW = 2
SLOTS = 10
PAIRS = 3
N_ROW = 16
N_COL = 32


def offset_choices(window, count):
    values = sorted(set(list(range(window)) + [count // 2, count - 1]))
    return values


def draw_offsets(key, count):
    values = offset_choices(WINDOW, count)
    table = jnp.array(values, dtype=jnp.int32)
    picks = jax.random.randint(key, (PAIRS, N_ROW, N_COL * SLOTS), 0, len(values)).astype(jnp.int32)
    offsets = table[picks]
    offsets = offsets.at[0, 0, 0].set(count // 2)
    offsets = offsets.at[0, 1, 0].set(count - 1)
    offsets = offsets.at[0, 2, 0].set(WINDOW - 1)
    return offsets.astype(jnp.int32)


def draw_block_target(key, part):
    offsets = draw_offsets(jax.random.fold_in(key, 11), N_ROW)
    rows_here = jnp.arange(N_ROW, dtype=jnp.int32)[None, :, None]
    return ((rows_here + offsets) % N_ROW).astype(jnp.int32)


def draw_block_source(key, part):
    offsets = draw_offsets(jax.random.fold_in(key, 23), N_COL)
    cols_here = (jnp.arange(N_COL * SLOTS, dtype=jnp.int32) // SLOTS)[None, None, :]
    return ((cols_here + offsets) % N_COL).astype(jnp.int32)


def level_of(key, dims, cuts, low, largest):
    loudness = 1.0
    for dim, parts in cuts:
        draws = jax.random.uniform(jax.random.fold_in(jax.random.fold_in(key, 6), dim), (parts,), jnp.float32, low / len(cuts), largest / len(cuts))
        loudness = loudness * jnp.repeat(jnp.exp(draws), dims[dim] // parts).reshape((-1,) + (1,) * (len(dims) - 1 - dim))
    return loudness


def centred(stream_key, shape, width, limit, cuts=(), held_as=jnp.bfloat16):
    values = jax.random.normal(stream_key, shape, jnp.float32) * width
    if len(cuts) > 0:
        values = level_of(stream_key, shape, cuts, -0.22, 0.18) * values
    return jnp.clip(values, min=-limit, max=limit).astype(held_as)


def setup_inputs(seed: int = 0) -> dict:
    key_list = jax.random.split(jax.random.key(seed), 6)
    rhs_panels = centred(key_list[0], (LEVELS, N_ROW, N_COL, NRHS, BS), 1.0, 6.0, ((1, 16), (2, 32)), jnp.float32)
    inverse_diag = centred(key_list[1], (LEVELS, N_ROW, N_COL, BS, BS), BS ** -0.5, 0.375, ((1, 16), (2, 32)))
    factor_blocks = centred(key_list[2], (PAIRS, N_ROW, N_COL * SLOTS, BS, BS), (2 * BS * SLOTS) ** -0.5, 0.078125, ((1, 16), (2, 32)))
    block_target = draw_block_target(jax.random.fold_in(key_list[5], 71), 0)
    block_source = draw_block_source(jax.random.fold_in(key_list[5], 71), 0)
    return {"rhs_panels": rhs_panels, "inverse_diag": inverse_diag, "factor_blocks": factor_blocks, "block_target": block_target, "block_source": block_source}


def pair_table(levels):
    return [(target_lvl, source_lvl) for target_lvl in range(1, levels) for source_lvl in range(target_lvl)]


def reference(rhs_panels, inverse_diag, factor_blocks, block_target, block_source):
    pair_list = pair_table(LEVELS)
    blocks = factor_blocks.reshape(PAIRS, N_ROW, N_COL, SLOTS, BS, BS)
    targets = block_target.reshape(PAIRS, N_ROW, N_COL, SLOTS).astype(jnp.int32)
    sources = block_source.reshape(PAIRS, N_ROW, N_COL, SLOTS).astype(jnp.int32)
    row_iota = jnp.arange(N_ROW, dtype=jnp.int32)
    col_iota = jnp.arange(N_COL, dtype=jnp.int32)
    forward = []
    forward_bf = []
    for current in range(LEVELS):
        residual = rhs_panels[current]
        if current > 0:
            chosen = [pair_idx for pair_idx, pair_info in enumerate(pair_list) if pair_info[0] == current]
            scanned_in = tuple((blocks[pair_idx], targets[pair_idx], sources[pair_idx], forward_bf[pair_list[pair_idx][1]]) for pair_idx in chosen)

            def step_row(running, scanned):
                term_sum = jnp.zeros((N_COL, N_ROW, NRHS, BS), jnp.float32)
                for row_blocks, row_targets, row_sources, row_panels in scanned:
                    picked = row_panels[row_sources]
                    products = jnp.einsum("csnb,csab->csna", picked.astype(jnp.float32), row_blocks.astype(jnp.float32), precision=lax.Precision.HIGHEST)
                    onehot = (row_targets[:, :, None] == row_iota[None, None, :]).astype(jnp.float32)
                    term_sum = term_sum + jnp.einsum("cst,csna->ctna", onehot, products, precision=lax.Precision.HIGHEST)
                rounded = lax.optimization_barrier(term_sum.astype(jnp.bfloat16)).astype(jnp.float32)
                return running + rounded, None

            total_init = jnp.zeros((N_COL, N_ROW, NRHS, BS), jnp.float32)
            summed, unused = lax.scan(step_row, total_init, scanned_in)
            residual = residual - jnp.transpose(summed, (1, 0, 2, 3))
        reduced = residual.astype(jnp.bfloat16)
        panel_now = jnp.einsum("rcnb,rcab->rcna", reduced.astype(jnp.float32), inverse_diag[current].astype(jnp.float32), precision=lax.Precision.HIGHEST)
        forward.append(panel_now)
        forward_bf.append(panel_now.astype(jnp.bfloat16))
    solutions = [None] * LEVELS
    backward_bf = [None] * LEVELS
    for current in reversed(range(LEVELS)):
        residual = forward[current]
        if current < LEVELS - 1:
            chosen = [pair_idx for pair_idx, pair_info in enumerate(pair_list) if pair_info[1] == current]
            dst_levels = [pair_list[pair_idx][0] for pair_idx in chosen]
            scanned_in = tuple((blocks[pair_idx], targets[pair_idx], sources[pair_idx]) for pair_idx in chosen)

            def back_row(scanned):
                term_sum = jnp.zeros((N_COL, N_COL, NRHS, BS), jnp.float32)
                for member, dst_level in zip(scanned, dst_levels):
                    row_blocks, row_targets, row_sources = member
                    picked = backward_bf[dst_level][row_targets, col_iota[:, None]]
                    products = jnp.einsum("csnb,csba->csna", picked.astype(jnp.float32), row_blocks.astype(jnp.float32), precision=lax.Precision.HIGHEST)
                    onehot = (row_sources[:, :, None] == col_iota[None, None, :]).astype(jnp.float32)
                    term_sum = term_sum + jnp.einsum("cse,csna->cena", onehot, products, precision=lax.Precision.HIGHEST)
                rounded = lax.optimization_barrier(term_sum.astype(jnp.bfloat16)).astype(jnp.float32)
                return jnp.sum(rounded, axis=0)

            summed = lax.map(back_row, scanned_in)
            residual = residual - summed
        reduced = residual.astype(jnp.bfloat16)
        answer = jnp.einsum("rcnb,rcba->rcna", reduced.astype(jnp.float32), inverse_diag[current].astype(jnp.float32), precision=lax.Precision.HIGHEST)
        solutions[current] = answer
        backward_bf[current] = answer.astype(jnp.bfloat16)
    return jnp.stack(solutions)
```

```python
import jax
import jax.numpy as jnp
from jax import lax
from jax.experimental import pallas as pl
from jax.experimental.pallas import tpu as pltpu
from jax.sharding import PartitionSpec as P

VMEM = pl.BlockSpec(memory_space=pltpu.VMEM)
SMEM = pl.BlockSpec(memory_space=pltpu.SMEM)
NT = (((1,), (1,)), ((), ()))
NN = (((1,), (0,)), ((), ()))
BF = jnp.bfloat16
F32 = jnp.float32


def pair_of(i, n):
    return i + 1 - 2 * (i % 2)


def cross_of(i, n):
    return (i - 1 + 2 * (i % 2) + n) % n


def far_of(i, n):
    return (i + n // 2) % n


def swap(value, axis, partner):
    n = lax.axis_size(axis)
    return lax.ppermute(value, axis, [(i, partner(i, n)) for i in range(n)])


def far_groups(n):
    half = n // 2
    return [[i, i + 1, i + half, i + half + 1] for i in range(0, half, 2)]


def gather_far(value, axis):
    return lax.all_gather(value, axis, axis_index_groups=far_groups(lax.axis_size(axis)))


def group_place(i, n):
    return i % 2 + 2 * (i // (n // 2))


def call(body, out_shape, in_specs, args, flops, moved, scratch=(), name=None, aliases=None, out_specs=None):
    return pl.pallas_call(
        body,
        out_shape=out_shape,
        in_specs=in_specs,
        out_specs=out_specs if out_specs is not None else jax.tree.map(lambda _: VMEM, out_shape),
        scratch_shapes=list(scratch),
        input_output_aliases=aliases or {},
        compiler_params=pltpu.CompilerParams(vmem_limit_bytes=16 * 2**20),
        cost_estimate=pl.CostEstimate(flops=flops, bytes_accessed=moved, transcendentals=0),
        name=name,
    )(*args)


def f32_like(x):
    return jax.ShapeDtypeStruct(x.shape, F32)


def bf_like(x):
    return jax.ShapeDtypeStruct(x.shape, BF)


def masked_sum(products, keys, key):
    total = None
    for s, k in enumerate(keys):
        term = jnp.where(k == key, products[s], 0.0)
        total = term if total is None else total + term
    return total


def product_body(kind, pair_idx, n_row, n_col, slots, add, finish):
    def body(*refs):
        targets, sources, blocks, *rest = refs
        count = 2 if kind == "fwd" else 4
        panels, rest = rest[:count], rest[count:]
        if add:
            base, rest = rest[0], rest[1:]
        outs, held, products = rest[:-2], rest[-2], rest[-1]
        r = lax.axis_index("row")
        c = lax.axis_index("col")
        if kind == "fwd":
            held[0:4] = panels[0][...]
            held[4] = panels[1][...]
        else:
            for i in range(4):
                held[i] = panels[i][...]
        keys = []
        for s in range(slots):
            t = targets[pair_idx, 0, s]
            e = sources[pair_idx, 0, s]
            if kind == "fwd":
                place = jnp.where(e == cross_of(c, n_col), 4, group_place(e, n_col))
                keys.append(t)
            else:
                place = jnp.where(
                    t == r, 0, jnp.where(t == pair_of(r, n_row), 1, jnp.where(t == far_of(r, n_row), 3, 2))
                )
                keys.append(e)
            products[s] = lax.dot_general(
                held[place], blocks[pair_idx, 0, s], NT if kind == "fwd" else NN, preferred_element_type=F32
            )
        me, n = (r, n_row) if kind == "fwd" else (c, n_col)
        for i, key in enumerate((me, pair_of(me, n), cross_of(me, n), far_of(me, n))):
            total = masked_sum(products, keys, key)
            if add:
                total = total + base[i]
            if finish:
                if kind == "fwd" or i in (0, 2):
                    outs[i if kind == "fwd" else i // 2][...] = total.astype(BF)
                else:
                    outs[2][i // 2] = total.astype(BF)
            else:
                outs[0][i] = total

    return body


def products(kind, pair_idx, tables, blocks, panels, base, finish):
    n_row, n_col = lax.axis_size("row"), lax.axis_size("col")
    slots, size = blocks.shape[2], blocks.shape[3]
    shape = panels[-1].shape
    panel = jax.ShapeDtypeStruct(shape, BF)
    if not finish:
        out = [jax.ShapeDtypeStruct((4, *shape), F32)]
    elif kind == "fwd":
        out = [panel] * 4
    else:
        out = [panel, panel, jax.ShapeDtypeStruct((2, *shape), BF)]
    args = [*tables, blocks, *panels] + ([base] if base is not None else [])
    return call(
        product_body(kind, pair_idx, n_row, n_col, slots, base is not None, finish),
        out,
        [SMEM, SMEM] + [VMEM] * (len(args) - 2),
        args,
        2 * slots * shape[0] * size * size,
        2 * slots * size * size,
        [pltpu.VMEM((5, *shape), BF), pltpu.VMEM((slots, *shape), F32)],
        f"{kind}{pair_idx}",
    )


def first_body(rhs, inverse, y_out, send_out):
    y = lax.dot_general(rhs[0, 0, 0].astype(BF), inverse[0, 0, 0], NT, preferred_element_type=F32)
    y_out[...] = y
    send_out[...] = y.astype(BF)


def forward_body(level, last):
    def body(rhs, inverse, own, pair, cross, far, *outs):
        total = own[...].astype(F32) + pair[...].astype(F32) + cross[...].astype(F32) + far[...].astype(F32)
        y = lax.dot_general(
            (rhs[level, 0, 0] - total).astype(BF), inverse[level, 0, 0], NT, preferred_element_type=F32
        )
        if last:
            y = lax.dot_general(y.astype(BF), inverse[level, 0, 0], NN, preferred_element_type=F32)
        outs[0][...] = y
        outs[1][...] = y.astype(BF)

    return body


def backward_body(level, n_col):
    def body(y, inverse, own, cross, group, *outs):
        c = lax.axis_index("col")
        total = (
            own[...].astype(F32)
            + cross[...].astype(F32)
            + group[group_place(pair_of(c, n_col), n_col), 0].astype(F32)
            + group[group_place(far_of(c, n_col), n_col), 1].astype(F32)
        )
        z = lax.dot_general((y[...] - total).astype(BF), inverse[level, 0, 0], NN, preferred_element_type=F32)
        outs[0][...] = z
        if level > 0:
            outs[1][...] = z.astype(BF)

    return body


def shards(rhs, inverse, blocks, targets, sources):
    n_col = lax.axis_size("col")
    tables = (targets, sources)
    panel = jax.ShapeDtypeStruct(rhs.shape[3:], F32)
    solve_flops = 2 * panel.shape[0] * panel.shape[1] ** 2

    def gather_cols(value):
        cross = swap(value, "col", cross_of)
        return [gather_far(value, "col"), cross]

    def gather_rows(value):
        far = swap(value, "row", far_of)
        pair = swap(value, "row", pair_of)
        cross = swap(value, "row", cross_of)
        return [value, pair, cross, far]

    def scatter_rows(parts):
        own, pair, cross, far = parts
        far = swap(far, "row", far_of)
        pair = swap(pair, "row", pair_of)
        cross = swap(cross, "row", cross_of)
        return [own, pair, cross, far]

    def scatter_cols(parts):
        own, cross, group = parts
        cross = swap(cross, "col", cross_of)
        return [own, cross, gather_far(group, "col")]

    y0, s0 = call(first_body, [panel, bf_like(panel)], [VMEM] * 2, (rhs, inverse), solve_flops, 2**18, name="y0")
    g0 = gather_cols(s0)
    parts = scatter_rows(products("fwd", 0, tables, blocks, g0, None, True))
    base2 = products("fwd", 1, tables, blocks, g0, None, False)[0]
    y1, s1 = call(
        forward_body(1, False), [panel, bf_like(panel)], [VMEM] * 6, (rhs, inverse, *parts), solve_flops, 2**18, name="y1"
    )
    g1 = gather_cols(s1)
    parts = scatter_rows(products("fwd", 2, tables, blocks, g1, base2, True))
    z2, b2 = call(
        forward_body(2, True), [panel, bf_like(panel)], [VMEM] * 6, (rhs, inverse, *parts), 2 * solve_flops, 2**18, name="z2"
    )
    h2 = gather_rows(b2)
    parts = scatter_cols(products("bwd", 2, tables, blocks, h2, None, True))
    base0 = products("bwd", 1, tables, blocks, h2, None, False)[0]
    z1, b1 = call(
        backward_body(1, n_col), [panel, bf_like(panel)], [VMEM] * 5, (y1, inverse, *parts), solve_flops, 2**18, name="z1"
    )
    h1 = gather_rows(b1)
    parts = scatter_cols(products("bwd", 0, tables, blocks, h1, base0, True))
    z0 = call(backward_body(0, n_col), [panel], [VMEM] * 5, (y0, inverse, *parts), solve_flops, 2**18, name="z0")[0]
    return jnp.stack([z0, z1, z2])[:, None, None]


def solution(mesh):
    placed = (
        P(None, "row", "col", None, None),
        P(None, "row", "col", None, None),
        P(None, "row", "col", None, None),
        P(None, "row", "col"),
        P(None, "row", "col"),
    )
    return jax.shard_map(
        shards,
        mesh=mesh,
        in_specs=placed,
        out_specs=P(None, "row", "col", None, None),
        check_vma=False,
    )
```

```python
import jax
import jax.numpy as jnp
from jax import lax
from jax.experimental import pallas as pl
from jax.experimental.pallas import tpu as pltpu
from jax.sharding import PartitionSpec as P

VMEM = pl.BlockSpec(memory_space=pltpu.VMEM)
SMEM = pl.BlockSpec(memory_space=pltpu.SMEM)
ANY = pl.BlockSpec(memory_space=pl.ANY)
HBM = pl.BlockSpec(memory_space=pltpu.HBM)
FIRST_FLOPS = 6 * 10**9
NT = (((1,), (1,)), ((), ()))
NN = (((1,), (0,)), ((), ()))
BF = jnp.bfloat16
F32 = jnp.float32


def pair_of(i, n):
    return i + 1 - 2 * (i % 2)


def cross_of(i, n):
    return (i - 1 + 2 * (i % 2) + n) % n


def far_of(i, n):
    return (i + n // 2) % n


def swap(value, axis, partner):
    n = lax.axis_size(axis)
    return lax.ppermute(value, axis, [(i, partner(i, n)) for i in range(n)])


def far_groups(n):
    half = n // 2
    return [[i, i + 1, i + half, i + half + 1] for i in range(0, half, 2)]


def gather_far(value, axis):
    return lax.all_gather(value, axis, axis_index_groups=far_groups(lax.axis_size(axis)))


def group_place(i, n):
    return i % 2 + 2 * (i // (n // 2))


def call(body, out_shape, in_specs, args, flops, moved, scratch=(), name=None, aliases=None, out_specs=None):
    return pl.pallas_call(
        body,
        out_shape=out_shape,
        in_specs=in_specs,
        out_specs=out_specs if out_specs is not None else jax.tree.map(lambda _: VMEM, out_shape),
        scratch_shapes=list(scratch),
        input_output_aliases=aliases or {},
        compiler_params=pltpu.CompilerParams(vmem_limit_bytes=16 * 2**20),
        cost_estimate=pl.CostEstimate(flops=flops, bytes_accessed=moved, transcendentals=0),
        name=name,
    )(*args)


def f32_like(x):
    return jax.ShapeDtypeStruct(x.shape, F32)


def bf_like(x):
    return jax.ShapeDtypeStruct(x.shape, BF)


def masked_sum(products, keys, key):
    total = None
    for s, k in enumerate(keys):
        term = jnp.where(k == key, products[s], 0.0)
        total = term if total is None else total + term
    return total


def product_body(kind, pair_idx, n_row, n_col, slots, add, finish):
    def body(*refs):
        targets, sources, blocks, *rest = refs
        count = 2 if kind == "fwd" else 4
        panels, rest = rest[:count], rest[count:]
        if add:
            base, rest = rest[0], rest[1:]
        outs, held, products = rest[:-2], rest[-2], rest[-1]
        r = lax.axis_index("row")
        c = lax.axis_index("col")
        if kind == "fwd":
            held[4] = panels[0][...]
            held[0:4] = panels[1][...]
        else:
            for i in range(4):
                held[i] = panels[i][...]
        keys = []
        for s in range(slots):
            t = targets[pair_idx, 0, s]
            e = sources[pair_idx, 0, s]
            if kind == "fwd":
                place = jnp.where(e == cross_of(c, n_col), 4, group_place(e, n_col))
                keys.append(t)
            else:
                place = jnp.where(
                    t == far_of(r, n_row), 0, jnp.where(t == pair_of(r, n_row), 1, jnp.where(t == r, 3, 2))
                )
                keys.append(e)
            products[s] = lax.dot_general(
                held[place], blocks[pair_idx, 0, s], NT if kind == "fwd" else NN, preferred_element_type=F32
            )
        me, n = (r, n_row) if kind == "fwd" else (c, n_col)
        for i, key in enumerate((me, pair_of(me, n), cross_of(me, n), far_of(me, n))):
            total = masked_sum(products, keys, key)
            if add:
                total = total + base[i]
            if finish:
                if kind == "fwd" or i in (0, 2):
                    outs[i if kind == "fwd" else i // 2][...] = total.astype(BF)
                else:
                    outs[2][i // 2] = total.astype(BF)
            else:
                outs[0][i] = total

    return body


def products(kind, pair_idx, tables, blocks, panels, base, finish):
    n_row, n_col = lax.axis_size("row"), lax.axis_size("col")
    slots, size = blocks.shape[2], blocks.shape[3]
    shape = panels[0].shape
    panel = jax.ShapeDtypeStruct(shape, BF)
    if not finish:
        out = [jax.ShapeDtypeStruct((4, *shape), F32)]
    elif kind == "fwd":
        out = [panel] * 4
    else:
        out = [panel, panel, jax.ShapeDtypeStruct((2, *shape), BF)]
    args = [*tables, blocks, *panels] + ([base] if base is not None else [])
    return call(
        product_body(kind, pair_idx, n_row, n_col, slots, base is not None, finish),
        out,
        [SMEM, SMEM] + [VMEM] * (len(args) - 2),
        args,
        2 * slots * shape[0] * size * size,
        2 * slots * size * size,
        [pltpu.VMEM((5, *shape), BF), pltpu.VMEM((slots, *shape), F32)],
        f"{kind}{pair_idx}",
    )


def first_body(rhs, inverse, y_out, send_out, rhs_held, inverse_held, sems):
    copies = [
        pltpu.make_async_copy(rhs.at[0, 0, 0], rhs_held, sems.at[0]),
        pltpu.make_async_copy(inverse.at[0, 0, 0], inverse_held, sems.at[1]),
    ]
    for copy in copies:
        copy.start()
    for copy in copies:
        copy.wait()
    y = lax.dot_general(rhs_held[...].astype(BF), inverse_held[...], NT, preferred_element_type=F32)
    y_out[...] = y
    send_out[...] = y.astype(BF)


def forward_body(level, last):
    def body(rhs, inverse, far, pair, cross, own, *outs):
        total = own[...].astype(F32) + pair[...].astype(F32) + cross[...].astype(F32) + far[...].astype(F32)
        y = lax.dot_general(
            (rhs[level, 0, 0] - total).astype(BF), inverse[level, 0, 0], NT, preferred_element_type=F32
        )
        if last:
            y = lax.dot_general(y.astype(BF), inverse[level, 0, 0], NN, preferred_element_type=F32)
        outs[0][...] = y
        outs[1][...] = y.astype(BF)

    return body


def backward_body(level, n_col):
    def body(y, inverse, own, cross, group, *outs):
        if level == 0:
            z1, z2, out, z0, sems = outs
            copies = [
                pltpu.make_async_copy(held, out.at[i, 0, 0], sems.at[i]) for i, held in enumerate((z0, z1, z2))
            ]
            copies[1].start()
            copies[2].start()
            outs = (z0,)
        c = lax.axis_index("col")
        total = (
            own[...].astype(F32)
            + cross[...].astype(F32)
            + group[group_place(pair_of(c, n_col), n_col), 0].astype(F32)
            + group[group_place(far_of(c, n_col), n_col), 1].astype(F32)
        )
        z = lax.dot_general((y[...] - total).astype(BF), inverse[level, 0, 0], NN, preferred_element_type=F32)
        outs[0][...] = z
        if level > 0:
            outs[1][...] = z.astype(BF)
        else:
            copies[0].start()
            for copy in copies:
                copy.wait()

    return body


def shards(rhs, inverse, blocks, targets, sources):
    n_col = lax.axis_size("col")
    tables = (targets, sources)
    panel = jax.ShapeDtypeStruct(rhs.shape[3:], F32)
    solve_flops = 2 * panel.shape[0] * panel.shape[1] ** 2

    def gather_cols(value):
        cross = swap(value, "col", cross_of)
        return [cross, gather_far(value, "col")]

    def gather_rows(value):
        far = swap(value, "row", far_of)
        pair = swap(value, "row", pair_of)
        cross = swap(value, "row", cross_of)
        return [far, pair, cross, value]

    def scatter_rows(parts):
        own, pair, cross, far = parts
        far = swap(far, "row", far_of)
        pair = swap(pair, "row", pair_of)
        cross = swap(cross, "row", cross_of)
        return [far, pair, cross, own]

    def scatter_cols(parts):
        own, cross, group = parts
        cross = swap(cross, "col", cross_of)
        return [own, cross, gather_far(group, "col")]

    y0, s0 = call(
        first_body,
        [panel, bf_like(panel)],
        [HBM] * 2,
        (rhs, inverse),
        FIRST_FLOPS,
        2**18,
        [pltpu.VMEM(panel.shape, F32), pltpu.VMEM(inverse.shape[3:], BF), pltpu.SemaphoreType.DMA((2,))],
        "y0",
    )
    g0 = gather_cols(s0)
    parts = scatter_rows(products("fwd", 0, tables, blocks, g0, None, True))
    base2 = products("fwd", 1, tables, blocks, g0, None, False)[0]
    y1, s1 = call(
        forward_body(1, False), [panel, bf_like(panel)], [VMEM] * 6, (rhs, inverse, *parts), solve_flops, 2**18, name="y1"
    )
    g1 = gather_cols(s1)
    parts = scatter_rows(products("fwd", 2, tables, blocks, g1, base2, True))
    z2, b2 = call(
        forward_body(2, True), [panel, bf_like(panel)], [VMEM] * 6, (rhs, inverse, *parts), 2 * solve_flops, 2**18, name="z2"
    )
    h2 = gather_rows(b2)
    parts = scatter_cols(products("bwd", 2, tables, blocks, h2, None, True))
    base0 = products("bwd", 1, tables, blocks, h2, None, False)[0]
    z1, b1 = call(
        backward_body(1, n_col), [panel, bf_like(panel)], [VMEM] * 5, (y1, inverse, *parts), solve_flops, 2**18, name="z1"
    )
    h1 = gather_rows(b1)
    parts = scatter_cols(products("bwd", 0, tables, blocks, h1, base0, True))
    return call(
        backward_body(0, n_col),
        f32_like(rhs),
        [VMEM] * 7,
        (y0, inverse, *parts, z1, z2),
        solve_flops,
        2**18,
        [pltpu.VMEM(panel.shape, F32), pltpu.SemaphoreType.DMA((3,))],
        "z0",
        out_specs=ANY,
    )


def solution(mesh):
    placed = (
        P(None, "row", "col", None, None),
        P(None, "row", "col", None, None),
        P(None, "row", "col", None, None),
        P(None, "row", "col"),
        P(None, "row", "col"),
    )
    return jax.shard_map(
        shards,
        mesh=mesh,
        in_specs=placed,
        out_specs=P(None, "row", "col", None, None),
        check_vma=False,
    )
```

```python
import jax
import jax.numpy as jnp
from jax import lax
from jax.experimental import pallas as pl
from jax.experimental.pallas import tpu as pltpu
from jax.sharding import PartitionSpec as P

VMEM = pl.BlockSpec(memory_space=pltpu.VMEM)
SMEM = pl.BlockSpec(memory_space=pltpu.SMEM)
ANY = pl.BlockSpec(memory_space=pl.ANY)
HBM = pl.BlockSpec(memory_space=pltpu.HBM)
EXCHANGE_FLOPS = 6 * 10**9
NT = (((1,), (1,)), ((), ()))
NN = (((1,), (0,)), ((), ()))
BF = jnp.bfloat16
F32 = jnp.float32


def pair_of(i, n):
    return i + 1 - 2 * (i % 2)


def cross_of(i, n):
    return (i - 1 + 2 * (i % 2) + n) % n


def far_of(i, n):
    return (i + n // 2) % n


def swap(value, axis, partner):
    n = lax.axis_size(axis)
    return lax.ppermute(value, axis, [(i, partner(i, n)) for i in range(n)])


def far_groups(n):
    half = n // 2
    return [[i, i + 1, i + half, i + half + 1] for i in range(0, half, 2)]


def gather_far(value, axis):
    return lax.all_gather(value, axis, axis_index_groups=far_groups(lax.axis_size(axis)))


def gather_pair(value, axis):
    pairs = [[i, i + 1] for i in range(0, lax.axis_size(axis), 2)]
    return lax.all_gather(value, axis, axis_index_groups=pairs)


def group_place(i, n):
    return i % 2 + 2 * (i // (n // 2))


def call(body, out_shape, in_specs, args, flops, moved, scratch=(), name=None, out_specs=None, vmem=16 * 2**20):
    return pl.pallas_call(
        body,
        out_shape=out_shape,
        in_specs=in_specs,
        out_specs=out_specs if out_specs is not None else jax.tree.map(lambda _: VMEM, out_shape),
        scratch_shapes=list(scratch),
        compiler_params=pltpu.CompilerParams(vmem_limit_bytes=vmem),
        cost_estimate=pl.CostEstimate(flops=flops, bytes_accessed=moved, transcendentals=0),
        name=name,
    )(*args)


def f32_like(x):
    return jax.ShapeDtypeStruct(x.shape, F32)


def bf_like(x):
    return jax.ShapeDtypeStruct(x.shape, BF)


def product_body(kind, index, pair_idx, n_row, n_col, slots, add, finish):
    def body(*refs):
        targets, sources, blocks, *rest = refs
        count = 2 if kind == "fwd" else 3
        panels, rest = rest[:count], rest[count:]
        if add:
            base, rest = rest[0], rest[1:]
        outs, held = rest[:-1], rest[-1]
        r = lax.axis_index("row")
        c = lax.axis_index("col")
        place = 0
        for panel in panels:
            if len(panel.shape) == 2:
                held[place] = panel[...]
                place += 1
            else:
                held[place : place + panel.shape[0]] = panel[...]
                place += panel.shape[0]
        me, n = (r, n_row) if kind == "fwd" else (c, n_col)
        kinds = (me, pair_of(me, n), cross_of(me, n), far_of(me, n))
        total = None
        for s in range(slots):
            t = targets[pair_idx, 0, s]
            e = sources[pair_idx, 0, s]
            if kind == "fwd":
                key = t
                place = jnp.where(e == cross_of(c, n_col), 0, 1 + group_place(e, n_col))
            else:
                key = e
                place = jnp.where(
                    t == far_of(r, n_row), 0, jnp.where(t == cross_of(r, n_row), 1, 2 + t % 2)
                )
            panel = held[place]
            zero = jnp.zeros_like(panel)
            stacked = jnp.concatenate([jnp.where(key == k, panel, zero) for k in kinds], axis=0)
            term = lax.dot_general(
                stacked, blocks[index, 0, s], NT if kind == "fwd" else NN, preferred_element_type=F32
            )
            total = term if total is None else total + term
        rows = held.shape[1]
        if add:
            total = total + base[...]
        if not finish:
            outs[0][...] = total
            return
        parts = [total[i * rows : (i + 1) * rows].astype(BF) for i in range(4)]
        if kind == "fwd":
            for out, part in zip(outs, parts):
                out[...] = part
        else:
            outs[0][...] = parts[0]
            outs[1][...] = parts[2]
            outs[2][0] = parts[1]
            outs[2][1] = parts[3]

    return body


def products(kind, index, pair_idx, tables, blocks, panels, base, finish):
    n_row, n_col = lax.axis_size("row"), lax.axis_size("col")
    slots, size = blocks.shape[2], blocks.shape[3]
    shape = panels[0].shape
    panel = jax.ShapeDtypeStruct(shape, BF)
    if not finish:
        out = [jax.ShapeDtypeStruct((4 * shape[0], shape[1]), F32)]
    elif kind == "fwd":
        out = [panel] * 4
    else:
        out = [panel, panel, jax.ShapeDtypeStruct((2, *shape), BF)]
    args = [*tables, blocks, *panels] + ([base] if base is not None else [])
    return call(
        product_body(kind, index, pair_idx, n_row, n_col, slots, base is not None, finish),
        out,
        [SMEM, SMEM] + [VMEM] * (len(args) - 2),
        args,
        8 * slots * shape[0] * size * size,
        2 * slots * size * size,
        [pltpu.VMEM((5 if kind == "fwd" else 4, *shape), BF)],
        f"{kind}{pair_idx}",
    )


def round_body(value, out):
    out[...] = value[...].astype(BF)


def forward_body(level, last):
    def body(rhs, inverse, far, cross, pairs, own, *outs):
        r = lax.axis_index("row")
        pair = pairs[1 - r % 2]
        total = own[...].astype(F32) + pair.astype(F32) + cross[...].astype(F32) + far[...].astype(F32)
        y = lax.dot_general(
            (rhs[level, 0, 0] - total).astype(BF), inverse[level, 0, 0], NT, preferred_element_type=F32
        )
        if last:
            y = lax.dot_general(y.astype(BF), inverse[level, 0, 0], NN, preferred_element_type=F32)
        outs[0][...] = y
        outs[1][...] = y.astype(BF)

    return body


def backward_body(level, n_col):
    def body(y, inverse, own, cross, group, *outs):
        if level == 0:
            z1, z2, out, z0, sems = outs
            copies = [
                pltpu.make_async_copy(held, out.at[i, 0, 0], sems.at[i]) for i, held in enumerate((z0, z1, z2))
            ]
            copies[1].start()
            copies[2].start()
            outs = (z0,)
        c = lax.axis_index("col")
        total = (
            own[...].astype(F32)
            + cross[...].astype(F32)
            + group[group_place(pair_of(c, n_col), n_col), 0].astype(F32)
            + group[group_place(far_of(c, n_col), n_col), 1].astype(F32)
        )
        z = lax.dot_general((y[...] - total).astype(BF), inverse[level, 0, 0], NN, preferred_element_type=F32)
        outs[0][...] = z
        if level > 0:
            outs[1][...] = z.astype(BF)
        else:
            copies[0].start()
            for copy in copies:
                copy.wait()

    return body


def shards(rhs, inverse, blocks, targets, sources):
    n_col = lax.axis_size("col")
    panel = jax.ShapeDtypeStruct(rhs.shape[3:], F32)
    solve_flops = 2 * panel.shape[0] * panel.shape[1] ** 2

    def gather_cols(value):
        cross = swap(value, "col", cross_of)
        return [cross, gather_far(value, "col")]

    def gather_rows(value):
        far = swap(value, "row", far_of)
        cross = swap(value, "row", cross_of)
        return [far, cross, gather_pair(value, "row")]

    def scatter_rows(parts):
        own, pair, cross, far = parts
        far = swap(far, "row", far_of)
        cross = swap(cross, "row", cross_of)
        return [far, cross, gather_pair(pair, "row"), own]

    def scatter_cols(parts):
        own, cross, group = parts
        cross = swap(cross, "col", cross_of)
        return [own, cross, gather_far(group, "col")]

    tables = (targets, sources)
    blocks0 = blocks
    y0 = lax.dot_general(rhs[0, 0, 0].astype(BF), inverse[0, 0, 0], NT, preferred_element_type=F32)
    s0 = call(round_body, bf_like(panel), [VMEM], (y0,), EXCHANGE_FLOPS, 2**17, name="s0")
    g0 = gather_cols(s0)
    parts = scatter_rows(products("fwd", 0, 0, tables, blocks0, g0, None, True))
    base2 = products("fwd", 1, 1, tables, blocks, g0, None, False)[0]
    y1, s1 = call(
        forward_body(1, False), [panel, bf_like(panel)], [VMEM] * 6, (rhs, inverse, *parts), solve_flops, 2**18, name="y1"
    )
    g1 = gather_cols(s1)
    parts = scatter_rows(products("fwd", 2, 2, tables, blocks, g1, base2, True))
    z2, b2 = call(
        forward_body(2, True), [panel, bf_like(panel)], [VMEM] * 6, (rhs, inverse, *parts), 2 * solve_flops, 2**18, name="z2"
    )
    h2 = gather_rows(b2)
    parts = scatter_cols(products("bwd", 2, 2, tables, blocks, h2, None, True))
    base0 = products("bwd", 1, 1, tables, blocks, h2, None, False)[0]
    z1, b1 = call(
        backward_body(1, n_col), [panel, bf_like(panel)], [VMEM] * 5, (y1, inverse, *parts), solve_flops, 2**18, name="z1"
    )
    h1 = gather_rows(b1)
    parts = scatter_cols(products("bwd", 0, 0, tables, blocks0, h1, base0, True))
    return call(
        backward_body(0, n_col),
        f32_like(rhs),
        [VMEM] * 7,
        (y0, inverse, *parts, z1, z2),
        solve_flops,
        2**18,
        [pltpu.VMEM(panel.shape, F32), pltpu.SemaphoreType.DMA((3,))],
        "z0",
        out_specs=ANY,
    )


def solution(mesh):
    placed = (
        P(None, "row", "col", None, None),
        P(None, "row", "col", None, None),
        P(None, "row", "col", None, None),
        P(None, "row", "col"),
        P(None, "row", "col"),
    )
    return jax.shard_map(
        shards,
        mesh=mesh,
        in_specs=placed,
        out_specs=P(None, "row", "col", None, None),
        check_vma=False,
    )
```

```python
import jax
import jax.numpy as jnp
from jax import lax
from jax.experimental import pallas as pl
from jax.experimental.pallas import tpu as pltpu
from jax.sharding import PartitionSpec as P


VMEM = pl.BlockSpec(memory_space=pltpu.VMEM)
ANY = pl.BlockSpec(memory_space=pl.ANY)
EXCHANGE_FLOPS = 6 * 10**9
NT = (((1,), (1,)), ((), ()))
NN = (((1,), (0,)), ((), ()))
BF = jnp.bfloat16
F32 = jnp.float32


def pair_of(i):
    return i + 1 - 2 * (i % 2)


def cross_of(i, n):
    return (i - 1 + 2 * (i % 2) + n) % n


def far_of(i, n):
    return (i + n // 2) % n


def swap(value, axis, partner):
    n = lax.axis_size(axis)
    return lax.ppermute(value, axis, [(i, partner(i, n)) for i in range(n)])


def far_groups(n):
    half = n // 2
    return [[i, i + 1, i + half, i + half + 1] for i in range(0, half, 2)]


def gather_far(value, axis):
    return lax.all_gather(value, axis, axis_index_groups=far_groups(lax.axis_size(axis)))


def gather_pair(value, axis):
    pairs = [[i, i + 1] for i in range(0, lax.axis_size(axis), 2)]
    return lax.all_gather(value, axis, axis_index_groups=pairs)


def group_place(i, n):
    return i % 2 + 2 * (i // (n // 2))


def call(body, out_shape, in_specs, args, flops, moved, scratch=(), out_specs=None, vmem=16 * 2**20):
    return pl.pallas_call(
        body,
        out_shape=out_shape,
        in_specs=in_specs,
        out_specs=out_specs if out_specs is not None else jax.tree.map(lambda _: VMEM, out_shape),
        scratch_shapes=list(scratch),
        compiler_params=pltpu.CompilerParams(vmem_limit_bytes=vmem),
        cost_estimate=pl.CostEstimate(flops=flops, bytes_accessed=moved, transcendentals=0),
    )(*args)


def f32_like(x):
    return jax.ShapeDtypeStruct(x.shape, F32)


def bf_like(x):
    return jax.ShapeDtypeStruct(x.shape, BF)


def splat(flags, s, shape):
    one = jnp.broadcast_to(flags[:, s : s + 1], (16, 128)).astype(BF)
    return jnp.tile(one, (shape[0] // 16, shape[1] // 128))


def pair_products(kind, pair_idx, n_row, n_col, slots, targets, sources, blocks, held):
    r = lax.axis_index("row")
    c = lax.axis_index("col")
    t = targets[pair_idx]
    e = sources[pair_idx]
    me, n, key = (r, n_row, t) if kind == "fwd" else (c, n_col, e)
    goals = [key == k for k in (me, pair_of(me), cross_of(me, n), far_of(me, n))]
    if kind == "fwd":
        low = c % (n_col // 2) - c % 2
        group = [low, low + 1, low + n_col // 2, low + n_col // 2 + 1]
        picks = [e == k for k in (cross_of(c, n_col), *group)]
    else:
        picks = [t == k for k in (far_of(r, n_row), cross_of(r, n_row), r - r % 2, r - r % 2 + 1)]
    goals = [g.astype(F32) for g in goals]
    picks = [g.astype(F32) for g in picks]
    shape = held[0].shape
    total = None
    for s in range(slots):
        panel = None
        for pick, one in zip(picks, held):
            term = splat(pick, s, shape) * one
            panel = term if panel is None else panel + term
        stacked = jnp.concatenate([splat(goal, s, shape) * panel for goal in goals], axis=0)
        term = lax.dot_general(
            stacked, blocks[pair_idx, 0, s], NT if kind == "fwd" else NN, preferred_element_type=F32
        )
        total = term if total is None else total + term
    return total


def product_body(kind, pair_idx, n_row, n_col, slots, add, extra):
    def body(*refs):
        targets, sources, blocks, *rest = refs
        count = 2 if kind == "fwd" else 3
        panels, rest = rest[:count], rest[count:]
        if add:
            base, rest = rest[0], rest[1:]
        outs = rest
        held = []
        for panel in panels:
            if len(panel.shape) == 2:
                held.append(panel[...])
            else:
                held.extend(panel[i] for i in range(panel.shape[0]))
        if pair_idx is not None:
            total = pair_products(kind, pair_idx, n_row, n_col, slots, targets, sources, blocks, held)
            if add:
                total = total + base[...]
            rows = held[0].shape[0]
            parts = [total[i * rows : (i + 1) * rows].astype(BF) for i in range(4)]
            if kind == "fwd":
                for out, part in zip(outs, parts):
                    out[...] = part
            else:
                outs[0][...] = parts[0]
                outs[1][...] = parts[2]
                outs[2][0] = parts[1]
                outs[2][1] = parts[3]
        if extra is not None:
            outs[-1][...] = pair_products(kind, extra, n_row, n_col, slots, targets, sources, blocks, held)

    return body


def products(kind, pair_idx, extra, tables, blocks, panels, base=None):
    n_row, n_col = lax.axis_size("row"), lax.axis_size("col")
    slots, size = blocks.shape[2], blocks.shape[3]
    shape = panels[0].shape
    panel = jax.ShapeDtypeStruct(shape, BF)
    out = []
    if pair_idx is not None:
        out = [panel] * 4 if kind == "fwd" else [panel, panel, jax.ShapeDtypeStruct((2, *shape), BF)]
    if extra is not None:
        out.append(jax.ShapeDtypeStruct((4 * shape[0], shape[1]), F32))
    args = [*tables, blocks, *panels] + ([base] if base is not None else [])
    pairs = len([p for p in (pair_idx, extra) if p is not None])
    return call(
        product_body(kind, pair_idx, n_row, n_col, slots, base is not None, extra),
        out,
        [VMEM] * len(args),
        args,
        8 * pairs * slots * shape[0] * size * size,
        2 * pairs * slots * size * size,
    )


def round_body(value, out):
    out[...] = value[...].astype(BF)


def forward_body(level, last):
    def body(rhs, inverse, far, cross, pairs, own, *outs):
        r = lax.axis_index("row")
        pair = pairs[1 - r % 2]
        total = own[...].astype(F32) + pair.astype(F32) + cross[...].astype(F32) + far[...].astype(F32)
        y = lax.dot_general(
            (rhs[level, 0, 0] - total).astype(BF), inverse[level, 0, 0], NT, preferred_element_type=F32
        )
        if last:
            y = lax.dot_general(y.astype(BF), inverse[level, 0, 0], NN, preferred_element_type=F32)
        outs[0][...] = y
        outs[1][...] = y.astype(BF)

    return body


def backward_body(level, n_col):
    def body(y, inverse, own, cross, group, *outs):
        if level == 0:
            z1, z2, out, z0, sems = outs
            copies = [
                pltpu.make_async_copy(held, out.at[i, 0, 0], sems.at[i]) for i, held in enumerate((z0, z1, z2))
            ]
            copies[1].start()
            copies[2].start()
            outs = (z0,)
        c = lax.axis_index("col")
        total = (
            own[...].astype(F32)
            + cross[...].astype(F32)
            + group[group_place(pair_of(c), n_col), 0].astype(F32)
            + group[group_place(far_of(c, n_col), n_col), 1].astype(F32)
        )
        z = lax.dot_general((y[...] - total).astype(BF), inverse[level, 0, 0], NN, preferred_element_type=F32)
        outs[0][...] = z
        if level > 0:
            outs[1][...] = z.astype(BF)
        else:
            copies[0].start()
            for copy in copies:
                copy.wait()

    return body


def shards(rhs, inverse, blocks, targets, sources):
    n_col = lax.axis_size("col")
    panel = jax.ShapeDtypeStruct(rhs.shape[3:], F32)
    solve_flops = 2 * panel.shape[0] * panel.shape[1] ** 2

    def gather_cols(value):
        cross = swap(value, "col", cross_of)
        return [cross, gather_far(value, "col")]

    def swap_rows(far, cross, pair):
        far = swap(far, "row", far_of)
        cross = swap(cross, "row", cross_of)
        return [far, cross, gather_pair(pair, "row")]

    def gather_rows(value):
        return swap_rows(value, value, value)

    def scatter_rows(parts):
        own, pair, cross, far = parts
        return [*swap_rows(far, cross, pair), own]

    def scatter_cols(parts):
        own, cross, group = parts
        cross = swap(cross, "col", cross_of)
        return [own, cross, gather_far(group, "col")]

    tables = (targets, sources)
    y0 = lax.dot_general(rhs[0, 0, 0].astype(BF), inverse[0, 0, 0], NT, preferred_element_type=F32)
    s0 = call(round_body, bf_like(panel), [VMEM], (y0,), EXCHANGE_FLOPS, 2**17)
    g0 = gather_cols(s0)
    parts = scatter_rows(products("fwd", 0, None, tables, blocks, g0))
    base2 = products("fwd", None, 1, tables, blocks, g0)[0]
    y1, s1 = call(
        forward_body(1, False), [panel, bf_like(panel)], [VMEM] * 6, (rhs, inverse, *parts), solve_flops, 2**18
    )
    g1 = gather_cols(s1)
    parts = scatter_rows(products("fwd", 2, None, tables, blocks, g1, base2))
    z2, b2 = call(
        forward_body(2, True), [panel, bf_like(panel)], [VMEM] * 6, (rhs, inverse, *parts), 2 * solve_flops, 2**18
    )
    *parts, base0 = products("bwd", 2, 1, tables, blocks, gather_rows(b2))
    parts = scatter_cols(parts)
    z1, b1 = call(
        backward_body(1, n_col), [panel, bf_like(panel)], [VMEM] * 5, (y1, inverse, *parts), solve_flops, 2**18
    )
    parts = scatter_cols(products("bwd", 0, None, tables, blocks, gather_rows(b1), base0))
    return call(
        backward_body(0, n_col),
        f32_like(rhs),
        [VMEM] * 7,
        (y0, inverse, *parts, z1, z2),
        solve_flops,
        2**18,
        [pltpu.VMEM(panel.shape, F32), pltpu.SemaphoreType.DMA((3,))],
        out_specs=ANY,
    )


def solution(mesh):
    placed = (
        P(None, "row", "col", None, None),
        P(None, "row", "col", None, None),
        P(None, "row", "col", None, None),
        P(None, "row", "col"),
        P(None, "row", "col"),
    )

    return jax.shard_map(
        shards,
        mesh=mesh,
        in_specs=placed,
        out_specs=P(None, "row", "col", None, None),
        check_vma=False,
    )
```

```python
import jax
import jax.numpy as jnp
from jax import lax
from jax.experimental import pallas as pl
from jax.experimental.pallas import tpu as pltpu
from jax.sharding import PartitionSpec as P


VMEM = pl.BlockSpec(memory_space=pltpu.VMEM)
ANY = pl.BlockSpec(memory_space=pl.ANY)
EXCHANGE_FLOPS = 6 * 10**9
NT = (((1,), (1,)), ((), ()))
NN = (((1,), (0,)), ((), ()))
BF = jnp.bfloat16
F32 = jnp.float32


def pair_of(i, n):
    return i + 1 - 2 * (i % 2)


def cross_of(i, n):
    return (i - 1 + 2 * (i % 2) + n) % n


def far_of(i, n):
    return (i + n // 2) % n


def swap(value, axis, partner):
    n = lax.axis_size(axis)
    return lax.ppermute(value, axis, [(i, partner(i, n)) for i in range(n)])


def far_groups(n):
    half = n // 2
    return [[i, i + 1, i + half, i + half + 1] for i in range(0, half, 2)]


def gather_far(value, axis):
    return lax.all_gather(value, axis, axis_index_groups=far_groups(lax.axis_size(axis)))


def gather_pair(value, axis):
    pairs = [[i, i + 1] for i in range(0, lax.axis_size(axis), 2)]
    return lax.all_gather(value, axis, axis_index_groups=pairs)


def group_place(i, n):
    return i % 2 + 2 * (i // (n // 2))


def call(body, out_shape, in_specs, args, flops, moved, scratch=(), out_specs=None, vmem=16 * 2**20):
    return pl.pallas_call(
        body,
        out_shape=out_shape,
        in_specs=in_specs,
        out_specs=out_specs if out_specs is not None else jax.tree.map(lambda _: VMEM, out_shape),
        scratch_shapes=list(scratch),
        compiler_params=pltpu.CompilerParams(vmem_limit_bytes=vmem),
        cost_estimate=pl.CostEstimate(flops=flops, bytes_accessed=moved, transcendentals=0),
    )(*args)


def f32_like(x):
    return jax.ShapeDtypeStruct(x.shape, F32)


def bf_like(x):
    return jax.ShapeDtypeStruct(x.shape, BF)


def splat(flags, s, shape):
    one = jnp.broadcast_to(flags[:, s : s + 1], (16, 128)).astype(BF)
    return jnp.tile(one, (shape[0] // 16, shape[1] // 128))


def pair_products(kind, pair_idx, n_row, n_col, slots, targets, sources, blocks, held):
    r = lax.axis_index("row")
    c = lax.axis_index("col")
    t = targets[pair_idx]
    e = sources[pair_idx]
    me, n, key = (r, n_row, t) if kind == "fwd" else (c, n_col, e)
    goals = [key == k for k in (me, pair_of(me, n), cross_of(me, n), far_of(me, n))]
    if kind == "fwd":
        low = c % (n_col // 2) - c % 2
        group = [low, low + 1, low + n_col // 2, low + n_col // 2 + 1]
        picks = [e == k for k in (cross_of(c, n_col), *group)]
    else:
        picks = [t == k for k in (far_of(r, n_row), cross_of(r, n_row), r - r % 2, r - r % 2 + 1)]
    goals = [g.astype(F32) for g in goals]
    picks = [g.astype(F32) for g in picks]
    shape = held[0].shape
    total = None
    for s in range(slots):
        panel = None
        for pick, one in zip(picks, held):
            term = splat(pick, s, shape) * one
            panel = term if panel is None else panel + term
        stacked = jnp.concatenate([splat(goal, s, shape) * panel for goal in goals], axis=0)
        term = lax.dot_general(
            stacked, blocks[pair_idx, 0, s], NT if kind == "fwd" else NN, preferred_element_type=F32
        )
        total = term if total is None else total + term
    return total


def product_body(kind, pair_idx, n_row, n_col, slots, add, extra, apart):
    def body(*refs):
        targets, sources, blocks, *rest = refs
        count = 2 if kind == "fwd" else 3
        panels, rest = rest[:count], rest[count:]
        if add:
            base, rest = rest[0], rest[1:]
        outs = rest
        held = []
        for panel in panels:
            if len(panel.shape) == 2:
                held.append(panel[...])
            else:
                held.extend(panel[i] for i in range(panel.shape[0]))
        if pair_idx is not None:
            total = pair_products(kind, pair_idx, n_row, n_col, slots, targets, sources, blocks, held)
            if add:
                total = total + base[...]
            rows = held[0].shape[0]
            parts = [total[i * rows : (i + 1) * rows].astype(BF) for i in range(4)]
            if apart:
                for out, part in zip(outs, parts):
                    out[...] = part
            else:
                outs[0][...] = parts[0]
                outs[1][...] = parts[2]
                outs[2][0] = parts[1]
                outs[2][1] = parts[3]
        if extra is not None:
            outs[-1][...] = pair_products(kind, extra, n_row, n_col, slots, targets, sources, blocks, held)

    return body


def products(kind, pair_idx, extra, tables, blocks, panels, base=None, apart=True):
    n_row, n_col = lax.axis_size("row"), lax.axis_size("col")
    slots, size = blocks.shape[2], blocks.shape[3]
    shape = panels[0].shape
    panel = jax.ShapeDtypeStruct(shape, BF)
    out = []
    if pair_idx is not None:
        out = [panel] * 4 if apart else [panel, panel, jax.ShapeDtypeStruct((2, *shape), BF)]
    if extra is not None:
        out.append(jax.ShapeDtypeStruct((4 * shape[0], shape[1]), F32))
    args = [*tables, blocks, *panels] + ([base] if base is not None else [])
    pairs = len([p for p in (pair_idx, extra) if p is not None])
    return call(
        product_body(kind, pair_idx, n_row, n_col, slots, base is not None, extra, apart),
        out,
        [VMEM] * len(args),
        args,
        8 * pairs * slots * shape[0] * size * size,
        2 * pairs * slots * size * size,
    )


def round_body(value, out):
    out[...] = value[...].astype(BF)


def forward_body(level, last):
    def body(rhs, inverse, far, cross, pairs, own, *outs):
        r = lax.axis_index("row")
        pair = pairs[1 - r % 2]
        total = own[...].astype(F32) + pair.astype(F32) + cross[...].astype(F32) + far[...].astype(F32)
        y = lax.dot_general(
            (rhs[level, 0, 0] - total).astype(BF), inverse[level, 0, 0], NT, preferred_element_type=F32
        )
        if last:
            y = lax.dot_general(y.astype(BF), inverse[level, 0, 0], NN, preferred_element_type=F32)
        outs[0][...] = y
        outs[1][...] = y.astype(BF)

    return body


def backward_body(n_col):
    def body(y, inverse, own, cross, group, z_out, send_out):
        c = lax.axis_index("col")
        total = (
            own[...].astype(F32)
            + cross[...].astype(F32)
            + group[group_place(pair_of(c, n_col), n_col), 0].astype(F32)
            + group[group_place(far_of(c, n_col), n_col), 1].astype(F32)
        )
        z = lax.dot_general((y[...] - total).astype(BF), inverse[1, 0, 0], NN, preferred_element_type=F32)
        z_out[...] = z
        send_out[...] = z.astype(BF)

    return body


def last_body(y, inverse, own, pair, far, cross, z1, z2, out, z0, sems):
    copies = [pltpu.make_async_copy(held, out.at[i, 0, 0], sems.at[i]) for i, held in enumerate((z0, z1, z2))]
    copies[1].start()
    copies[2].start()
    total = own[...].astype(F32) + pair[...].astype(F32) + far[...].astype(F32) + cross[...].astype(F32)
    z0[...] = lax.dot_general((y[...] - total).astype(BF), inverse[0, 0, 0], NN, preferred_element_type=F32)
    copies[0].start()
    for copy in copies:
        copy.wait()


def shards(rhs, inverse, blocks, targets, sources):
    n_col = lax.axis_size("col")
    panel = jax.ShapeDtypeStruct(rhs.shape[3:], F32)
    solve_flops = 2 * panel.shape[0] * panel.shape[1] ** 2

    def gather_cols(value):
        cross = swap(value, "col", cross_of)
        return [cross, gather_far(value, "col")]

    def swap_rows(far, cross, pair):
        far = swap(far, "row", far_of)
        cross = swap(cross, "row", cross_of)
        return [far, cross, gather_pair(pair, "row")]

    def gather_rows(value):
        return swap_rows(value, value, value)

    def scatter_rows(parts):
        own, pair, cross, far = parts
        return [*swap_rows(far, cross, pair), own]

    def last_scatter(parts):
        own, pair, cross, far = parts
        pair = swap(pair, "col", pair_of)
        far = swap(far, "col", far_of)
        cross = swap(cross, "col", cross_of)
        return [own, pair, far, cross]

    def scatter_cols(parts):
        own, cross, group = parts
        cross = swap(cross, "col", cross_of)
        return [own, cross, gather_far(group, "col")]

    tables = (targets, sources)
    y0 = lax.dot_general(rhs[0, 0, 0].astype(BF), inverse[0, 0, 0], NT, preferred_element_type=F32)
    s0 = call(round_body, bf_like(panel), [VMEM], (y0,), EXCHANGE_FLOPS, 2**17)
    g0 = gather_cols(s0)
    parts = scatter_rows(products("fwd", 0, None, tables, blocks, g0))
    base2 = products("fwd", None, 1, tables, blocks, g0)[0]
    y1, s1 = call(
        forward_body(1, False), [panel, bf_like(panel)], [VMEM] * 6, (rhs, inverse, *parts), solve_flops, 2**18
    )
    g1 = gather_cols(s1)
    parts = scatter_rows(products("fwd", 2, None, tables, blocks, g1, base2))
    z2, b2 = call(
        forward_body(2, True), [panel, bf_like(panel)], [VMEM] * 6, (rhs, inverse, *parts), 2 * solve_flops, 2**18
    )
    *parts, base0 = products("bwd", 2, 1, tables, blocks, gather_rows(b2), apart=False)
    parts = scatter_cols(parts)
    z1, b1 = call(backward_body(n_col), [panel, bf_like(panel)], [VMEM] * 5, (y1, inverse, *parts), solve_flops, 2**18)
    parts = last_scatter(products("bwd", 0, None, tables, blocks, gather_rows(b1), base0))
    return call(
        last_body,
        f32_like(rhs),
        [VMEM] * 8,
        (y0, inverse, *parts, z1, z2),
        solve_flops,
        2**18,
        [pltpu.VMEM(panel.shape, F32), pltpu.SemaphoreType.DMA((3,))],
        out_specs=ANY,
    )


def solution(mesh):
    placed = (
        P(None, "row", "col", None, None),
        P(None, "row", "col", None, None),
        P(None, "row", "col", None, None),
        P(None, "row", "col"),
        P(None, "row", "col"),
    )

    return jax.shard_map(
        shards,
        mesh=mesh,
        in_specs=placed,
        out_specs=P(None, "row", "col", None, None),
        check_vma=False,
    )
```

```python
import jax
import jax.numpy as jnp
from jax import lax
from jax.experimental import pallas as pl
from jax.experimental.pallas import tpu as pltpu
from jax.sharding import PartitionSpec as P


VMEM = pl.BlockSpec(memory_space=pltpu.VMEM)
ANY = pl.BlockSpec(memory_space=pl.ANY)
EXCHANGE_FLOPS = 6 * 10**9
NT = (((1,), (1,)), ((), ()))
NN = (((1,), (0,)), ((), ()))
BF = jnp.bfloat16
F32 = jnp.float32


def pair_of(i):
    return i + 1 - 2 * (i % 2)


def cross_of(i, n):
    return (i - 1 + 2 * (i % 2) + n) % n


def far_of(i, n):
    return (i + n // 2) % n


def swap(value, axis, partner):
    n = lax.axis_size(axis)
    return lax.ppermute(value, axis, [(i, partner(i, n)) for i in range(n)])


def far_groups(n):
    half = n // 2
    return [[i, i + 1, i + half, i + half + 1] for i in range(0, half, 2)]


def gather_far(value, axis):
    return lax.all_gather(value, axis, axis_index_groups=far_groups(lax.axis_size(axis)))


def gather_pair(value, axis):
    pairs = [[i, i + 1] for i in range(0, lax.axis_size(axis), 2)]
    return lax.all_gather(value, axis, axis_index_groups=pairs)


def call(body, out_shape, in_specs, args, flops, moved, scratch=(), out_specs=None, vmem=16 * 2**20):
    return pl.pallas_call(
        body,
        out_shape=out_shape,
        in_specs=in_specs,
        out_specs=out_specs if out_specs is not None else jax.tree.map(lambda _: VMEM, out_shape),
        scratch_shapes=list(scratch),
        compiler_params=pltpu.CompilerParams(vmem_limit_bytes=vmem),
        cost_estimate=pl.CostEstimate(flops=flops, bytes_accessed=moved, transcendentals=0),
    )(*args)


def f32_like(x):
    return jax.ShapeDtypeStruct(x.shape, F32)


def bf_like(x):
    return jax.ShapeDtypeStruct(x.shape, BF)


def splat(flags, s, shape):
    one = jnp.broadcast_to(flags[:, s : s + 1], (16, 128)).astype(BF)
    return jnp.tile(one, (shape[0] // 16, shape[1] // 128))


def pair_products(kind, pair_idx, n_row, n_col, slots, targets, sources, blocks, held):
    r = lax.axis_index("row")
    c = lax.axis_index("col")
    t = targets[pair_idx]
    e = sources[pair_idx]
    me, n, key = (r, n_row, t) if kind == "fwd" else (c, n_col, e)
    goals = [key == k for k in (me, pair_of(me), cross_of(me, n), far_of(me, n))]
    if kind == "fwd":
        low = c % (n_col // 2) - c % 2
        group = [low, low + 1, low + n_col // 2, low + n_col // 2 + 1]
        picks = [e == k for k in (cross_of(c, n_col), *group)]
    else:
        picks = [t == k for k in (far_of(r, n_row), cross_of(r, n_row), r - r % 2, r - r % 2 + 1)]
    goals = [g.astype(F32) for g in goals]
    picks = [g.astype(F32) for g in picks]
    shape = held[0].shape
    total = None
    for s in range(slots):
        panel = None
        for pick, one in zip(picks, held):
            term = splat(pick, s, shape) * one
            panel = term if panel is None else panel + term
        stacked = jnp.concatenate([splat(goal, s, shape) * panel for goal in goals], axis=0)
        term = lax.dot_general(
            stacked, blocks[pair_idx, 0, s], NT if kind == "fwd" else NN, preferred_element_type=F32
        )
        total = term if total is None else total + term
    return total


def product_body(kind, pair_idx, n_row, n_col, slots, add, extra, apart):
    def body(*refs):
        targets, sources, blocks, *rest = refs
        count = 2 if kind == "fwd" else 3
        panels, rest = rest[:count], rest[count:]
        if add:
            base, rest = rest[0], rest[1:]
        outs = rest
        held = []
        for panel in panels:
            if len(panel.shape) == 2:
                held.append(panel[...])
            else:
                held.extend(panel[i] for i in range(panel.shape[0]))
        if pair_idx is not None:
            total = pair_products(kind, pair_idx, n_row, n_col, slots, targets, sources, blocks, held)
            if add:
                total = total + base[...]
            rows = held[0].shape[0]
            parts = [total[i * rows : (i + 1) * rows].astype(BF) for i in range(4)]
            if apart:
                for out, part in zip(outs, parts):
                    out[...] = part
            else:
                outs[0][...] = parts[0]
                outs[1][...] = parts[2]
                outs[2][0] = parts[1]
                outs[2][1] = parts[3]
        if extra is not None:
            outs[-1][...] = pair_products(kind, extra, n_row, n_col, slots, targets, sources, blocks, held)

    return body


def products(kind, pair_idx, extra, tables, blocks, panels, base=None, apart=True):
    n_row, n_col = lax.axis_size("row"), lax.axis_size("col")
    slots, size = blocks.shape[2], blocks.shape[3]
    shape = panels[0].shape
    panel = jax.ShapeDtypeStruct(shape, BF)
    out = []
    if pair_idx is not None:
        out = [panel] * 4 if apart else [panel, panel, jax.ShapeDtypeStruct((2, *shape), BF)]
    if extra is not None:
        out.append(jax.ShapeDtypeStruct((4 * shape[0], shape[1]), F32))
    args = [*tables, blocks, *panels] + ([base] if base is not None else [])
    pairs = len([p for p in (pair_idx, extra) if p is not None])
    return call(
        product_body(kind, pair_idx, n_row, n_col, slots, base is not None, extra, apart),
        out,
        [VMEM] * len(args),
        args,
        8 * pairs * slots * shape[0] * size * size,
        2 * pairs * slots * size * size,
    )


def round_body(value, out):
    out[...] = value[...].astype(BF)


def forward_body(level, last):
    def body(rhs, inverse, far, cross, pairs, own, *outs):
        r = lax.axis_index("row")
        pair = pairs[1 - r % 2]
        total = own[...].astype(F32) + pair.astype(F32) + cross[...].astype(F32) + far[...].astype(F32)
        y = lax.dot_general(
            (rhs[level, 0, 0] - total).astype(BF), inverse[level, 0, 0], NT, preferred_element_type=F32
        )
        if last:
            y = lax.dot_general(y.astype(BF), inverse[level, 0, 0], NN, preferred_element_type=F32)
        outs[0][...] = y
        outs[1][...] = y.astype(BF)

    return body


def backward_body():
    def body(y, inverse, own, pair, far, cross, z_out, send_out):
        other = pair[1 - lax.axis_index("col") % 2]
        total = own[...].astype(F32) + other.astype(F32) + far[...].astype(F32) + cross[...].astype(F32)
        z = lax.dot_general((y[...] - total).astype(BF), inverse[1, 0, 0], NN, preferred_element_type=F32)
        z_out[...] = z
        send_out[...] = z.astype(BF)

    return body


def last_body(y, inverse, own, pair, far, cross, z1, z2, out, z0, sems):
    copies = [pltpu.make_async_copy(held, out.at[i, 0, 0], sems.at[i]) for i, held in enumerate((z0, z1, z2))]
    copies[1].start()
    copies[2].start()
    other = pair[1 - lax.axis_index("col") % 2]
    total = own[...].astype(F32) + other.astype(F32) + far[...].astype(F32) + cross[...].astype(F32)
    z0[...] = lax.dot_general((y[...] - total).astype(BF), inverse[0, 0, 0], NN, preferred_element_type=F32)
    copies[0].start()
    for copy in copies:
        copy.wait()


def shards(rhs, inverse, blocks, targets, sources):
    panel = jax.ShapeDtypeStruct(rhs.shape[3:], F32)
    solve_flops = 2 * panel.shape[0] * panel.shape[1] ** 2

    def gather_cols(value):
        cross = swap(value, "col", cross_of)
        return [cross, gather_far(value, "col")]

    def swap_rows(far, cross, pair):
        far = swap(far, "row", far_of)
        cross = swap(cross, "row", cross_of)
        return [far, cross, gather_pair(pair, "row")]

    def gather_rows(value):
        return swap_rows(value, value, value)

    def scatter_rows(parts):
        own, pair, cross, far = parts
        return [*swap_rows(far, cross, pair), own]

    def last_scatter(parts):
        own, pair, cross, far = parts
        cross = swap(cross, "col", cross_of)
        far = swap(far, "col", far_of)
        pair = gather_pair(pair, "col")
        return [own, pair, far, cross]

    tables = (targets, sources)
    y0 = lax.dot_general(rhs[0, 0, 0].astype(BF), inverse[0, 0, 0], NT, preferred_element_type=F32)
    s0 = call(round_body, bf_like(panel), [VMEM], (y0,), EXCHANGE_FLOPS, 2**17)
    g0 = gather_cols(s0)
    parts = scatter_rows(products("fwd", 0, None, tables, blocks, g0))
    base2 = products("fwd", None, 1, tables, blocks, g0)[0]
    y1, s1 = call(
        forward_body(1, False), [panel, bf_like(panel)], [VMEM] * 6, (rhs, inverse, *parts), solve_flops, 2**18
    )
    g1 = gather_cols(s1)
    parts = scatter_rows(products("fwd", 2, None, tables, blocks, g1, base2))
    z2, b2 = call(
        forward_body(2, True), [panel, bf_like(panel)], [VMEM] * 6, (rhs, inverse, *parts), 2 * solve_flops, 2**18
    )
    h2 = gather_rows(b2)
    parts = last_scatter(products("bwd", 2, None, tables, blocks, h2))
    base0 = products("bwd", None, 1, tables, blocks, h2)[0]
    z1, b1 = call(backward_body(), [panel, bf_like(panel)], [VMEM] * 6, (y1, inverse, *parts), solve_flops, 2**18)
    parts = last_scatter(products("bwd", 0, None, tables, blocks, gather_rows(b1), base0))
    return call(
        last_body,
        f32_like(rhs),
        [VMEM] * 8,
        (y0, inverse, *parts, z1, z2),
        solve_flops,
        2**18,
        [pltpu.VMEM(panel.shape, F32), pltpu.SemaphoreType.DMA((3,))],
        out_specs=ANY,
    )


def solution(mesh):
    placed = (
        P(None, "row", "col", None, None),
        P(None, "row", "col", None, None),
        P(None, "row", "col", None, None),
        P(None, "row", "col"),
        P(None, "row", "col"),
    )

    return jax.shard_map(
        shards,
        mesh=mesh,
        in_specs=placed,
        out_specs=P(None, "row", "col", None, None),
        check_vma=False,
    )
```

```python
import jax
import jax.numpy as jnp
from jax import lax
from jax.experimental import pallas as pl
from jax.experimental.pallas import tpu as pltpu
from jax.sharding import PartitionSpec as P


VMEM = pl.BlockSpec(memory_space=pltpu.VMEM)
ANY = pl.BlockSpec(memory_space=pl.ANY)
EXCHANGE_FLOPS = 6 * 10**9
NT = (((1,), (1,)), ((), ()))
NN = (((1,), (0,)), ((), ()))
BF = jnp.bfloat16
F32 = jnp.float32


def pair_of(i):
    return i + 1 - 2 * (i % 2)


def cross_of(i, n):
    return (i - 1 + 2 * (i % 2) + n) % n


def far_of(i, n):
    return (i + n // 2) % n


def swap(value, axis, partner):
    n = lax.axis_size(axis)
    return lax.ppermute(value, axis, [(i, partner(i, n)) for i in range(n)])


def gather_pair(value, axis):
    pairs = [[i, i + 1] for i in range(0, lax.axis_size(axis), 2)]
    return lax.all_gather(value, axis, axis_index_groups=pairs)


def call(body, out_shape, in_specs, args, flops, moved, scratch=(), out_specs=None, vmem=16 * 2**20):
    return pl.pallas_call(
        body,
        out_shape=out_shape,
        in_specs=in_specs,
        out_specs=out_specs if out_specs is not None else jax.tree.map(lambda _: VMEM, out_shape),
        scratch_shapes=list(scratch),
        compiler_params=pltpu.CompilerParams(vmem_limit_bytes=vmem),
        cost_estimate=pl.CostEstimate(flops=flops, bytes_accessed=moved, transcendentals=0),
    )(*args)


def f32_like(x):
    return jax.ShapeDtypeStruct(x.shape, F32)


def bf_like(x):
    return jax.ShapeDtypeStruct(x.shape, BF)


def splat(flags, s, shape):
    one = jnp.broadcast_to(flags[:, s : s + 1], (16, 128)).astype(BF)
    return jnp.tile(one, (shape[0] // 16, shape[1] // 128))


def pair_products(kind, pair_idx, n_row, n_col, slots, targets, sources, blocks, held):
    r = lax.axis_index("row")
    c = lax.axis_index("col")
    t = targets[pair_idx]
    e = sources[pair_idx]
    me, n, key = (r, n_row, t) if kind == "fwd" else (c, n_col, e)
    goals = [key == k for k in (me, pair_of(me), cross_of(me, n), far_of(me, n))]
    if kind == "fwd":
        picks = [e == k for k in (cross_of(c, n_col), far_of(c, n_col), c - c % 2, c - c % 2 + 1)]
    else:
        picks = [t == k for k in (far_of(r, n_row), cross_of(r, n_row), r - r % 2, r - r % 2 + 1)]
    goals = [g.astype(F32) for g in goals]
    picks = [g.astype(F32) for g in picks]
    shape = held[0].shape
    total = None
    for s in range(slots):
        panel = None
        for pick, one in zip(picks, held):
            term = splat(pick, s, shape) * one
            panel = term if panel is None else panel + term
        stacked = jnp.concatenate([splat(goal, s, shape) * panel for goal in goals], axis=0)
        term = lax.dot_general(
            stacked, blocks[pair_idx, 0, s], NT if kind == "fwd" else NN, preferred_element_type=F32
        )
        total = term if total is None else total + term
    return total


def product_body(kind, pair_idx, n_row, n_col, slots, add, extra, apart):
    def body(*refs):
        targets, sources, blocks, *rest = refs
        count = 3
        panels, rest = rest[:count], rest[count:]
        if add:
            base, rest = rest[0], rest[1:]
        outs = rest
        held = []
        for panel in panels:
            if len(panel.shape) == 2:
                held.append(panel[...])
            else:
                held.extend(panel[i] for i in range(panel.shape[0]))
        if pair_idx is not None:
            total = pair_products(kind, pair_idx, n_row, n_col, slots, targets, sources, blocks, held)
            if add:
                total = total + base[...]
            rows = held[0].shape[0]
            parts = [total[i * rows : (i + 1) * rows].astype(BF) for i in range(4)]
            if apart:
                for out, part in zip(outs, parts):
                    out[...] = part
            else:
                outs[0][...] = parts[0]
                outs[1][...] = parts[2]
                outs[2][0] = parts[1]
                outs[2][1] = parts[3]
        if extra is not None:
            outs[-1][...] = pair_products(kind, extra, n_row, n_col, slots, targets, sources, blocks, held)

    return body


def products(kind, pair_idx, extra, tables, blocks, panels, base=None, apart=True):
    n_row, n_col = lax.axis_size("row"), lax.axis_size("col")
    slots, size = blocks.shape[2], blocks.shape[3]
    shape = panels[0].shape
    panel = jax.ShapeDtypeStruct(shape, BF)
    out = []
    if pair_idx is not None:
        out = [panel] * 4 if apart else [panel, panel, jax.ShapeDtypeStruct((2, *shape), BF)]
    if extra is not None:
        out.append(jax.ShapeDtypeStruct((4 * shape[0], shape[1]), F32))
    args = [*tables, blocks, *panels] + ([base] if base is not None else [])
    pairs = len([p for p in (pair_idx, extra) if p is not None])
    return call(
        product_body(kind, pair_idx, n_row, n_col, slots, base is not None, extra, apart),
        out,
        [VMEM] * len(args),
        args,
        8 * pairs * slots * shape[0] * size * size,
        2 * pairs * slots * size * size,
    )


def round_body(value, out):
    out[...] = value[...].astype(BF)


def forward_body(level, last):
    def body(rhs, inverse, far, cross, pairs, own, *outs):
        r = lax.axis_index("row")
        pair = pairs[1 - r % 2]
        total = own[...].astype(F32) + pair.astype(F32) + cross[...].astype(F32) + far[...].astype(F32)
        y = lax.dot_general(
            (rhs[level, 0, 0] - total).astype(BF), inverse[level, 0, 0], NT, preferred_element_type=F32
        )
        if last:
            y = lax.dot_general(y.astype(BF), inverse[level, 0, 0], NN, preferred_element_type=F32)
        outs[0][...] = y
        outs[1][...] = y.astype(BF)

    return body


def backward_body():
    def body(y, inverse, own, pair, far, cross, z_out, send_out):
        other = pair[1 - lax.axis_index("col") % 2]
        total = own[...].astype(F32) + other.astype(F32) + far[...].astype(F32) + cross[...].astype(F32)
        z = lax.dot_general((y[...] - total).astype(BF), inverse[1, 0, 0], NN, preferred_element_type=F32)
        z_out[...] = z
        send_out[...] = z.astype(BF)

    return body


def last_body(y, inverse, own, pair, far, cross, z1, z2, out, z0, sems):
    copies = [pltpu.make_async_copy(held, out.at[i, 0, 0], sems.at[i]) for i, held in enumerate((z0, z1, z2))]
    copies[1].start()
    copies[2].start()
    other = pair[1 - lax.axis_index("col") % 2]
    total = own[...].astype(F32) + other.astype(F32) + far[...].astype(F32) + cross[...].astype(F32)
    z0[...] = lax.dot_general((y[...] - total).astype(BF), inverse[0, 0, 0], NN, preferred_element_type=F32)
    copies[0].start()
    for copy in copies:
        copy.wait()


def shards(rhs, inverse, blocks, targets, sources):
    panel = jax.ShapeDtypeStruct(rhs.shape[3:], F32)
    solve_flops = 2 * panel.shape[0] * panel.shape[1] ** 2

    def gather_cols(value):
        cross = swap(value, "col", cross_of)
        far = swap(value, "col", far_of)
        return [cross, far, gather_pair(value, "col")]

    def swap_rows(far, cross, pair):
        far = swap(far, "row", far_of)
        cross = swap(cross, "row", cross_of)
        return [far, cross, gather_pair(pair, "row")]

    def gather_rows(value):
        return swap_rows(value, value, value)

    def scatter_rows(parts):
        own, pair, cross, far = parts
        return [*swap_rows(far, cross, pair), own]

    def last_scatter(parts):
        own, pair, cross, far = parts
        cross = swap(cross, "col", cross_of)
        far = swap(far, "col", far_of)
        pair = gather_pair(pair, "col")
        return [own, pair, far, cross]

    tables = (targets, sources)
    y0 = lax.dot_general(rhs[0, 0, 0].astype(BF), inverse[0, 0, 0], NT, preferred_element_type=F32)
    s0 = call(round_body, bf_like(panel), [VMEM], (y0,), EXCHANGE_FLOPS, 2**17)
    g0 = gather_cols(s0)
    parts = scatter_rows(products("fwd", 0, None, tables, blocks, g0))
    base2 = products("fwd", None, 1, tables, blocks, g0)[0]
    y1, s1 = call(
        forward_body(1, False), [panel, bf_like(panel)], [VMEM] * 6, (rhs, inverse, *parts), solve_flops, 2**18
    )
    g1 = gather_cols(s1)
    parts = scatter_rows(products("fwd", 2, None, tables, blocks, g1, base2))
    z2, b2 = call(
        forward_body(2, True), [panel, bf_like(panel)], [VMEM] * 6, (rhs, inverse, *parts), 2 * solve_flops, 2**18
    )
    h2 = gather_rows(b2)
    parts = last_scatter(products("bwd", 2, None, tables, blocks, h2))
    base0 = products("bwd", None, 1, tables, blocks, h2)[0]
    z1, b1 = call(backward_body(), [panel, bf_like(panel)], [VMEM] * 6, (y1, inverse, *parts), solve_flops, 2**18)
    parts = last_scatter(products("bwd", 0, None, tables, blocks, gather_rows(b1), base0))
    return call(
        last_body,
        f32_like(rhs),
        [VMEM] * 8,
        (y0, inverse, *parts, z1, z2),
        solve_flops,
        2**18,
        [pltpu.VMEM(panel.shape, F32), pltpu.SemaphoreType.DMA((3,))],
        out_specs=ANY,
    )


def solution(mesh):
    placed = (
        P(None, "row", "col", None, None),
        P(None, "row", "col", None, None),
        P(None, "row", "col", None, None),
        P(None, "row", "col"),
        P(None, "row", "col"),
    )

    return jax.shard_map(
        shards,
        mesh=mesh,
        in_specs=placed,
        out_specs=P(None, "row", "col", None, None),
        check_vma=False,
    )
```
